32 devices in a mesh: dp: 4 (over z), fsdp: 8 (over y, x, core).
Axes of the slice: x: 2, y: 2, z: 4, core: 2. Of those that a mesh axis runs over, the one named last changes fastest.
Arguments:
- replica_grads: bfloat16 [4, 8192, 4096], P('dp', 'fsdp'), may hold values from -4 to 4
- slot_table: int32 [32], replicated, may hold values from 0 to 39, as said below
- left_gram_state: float32 [40, 1, 4, 256, 1024], P('fsdp', None, 'dp')
- right_gram_state: float32 [40, 1, 4, 256, 1024], P('fsdp', None, 'dp')
- left_inverse_root: bfloat16 [40, 1, 4, 256, 1024], P('fsdp', None, 'dp')
- right_inverse_root: bfloat16 [40, 1, 4, 256, 1024], P('fsdp', None, 'dp')
Outputs:
- direction: bfloat16 [8, 4, 256, 4096], P('fsdp', 'dp')
- left_new: float32 [40, 1, 4, 256, 1024], P('fsdp', None, 'dp')
- right_new: float32 [40, 1, 4, 256, 1024], P('fsdp', None, 'dp')
The draws below stay inside these ranges and needn't reach their ends.
Inputs may be any that keep to these rules, and one draw needn't show every extreme that they name: `slot_table`: the entries are distinct; slot v belongs to owner v // 5 of the flat shards' devices; some owner holds 5 blocks.
All inputs are finite; a program needn't handle non-finite values.
Results may differ from the reference program's by a relative error of at most 0.02.
Values may be sent and summed in bfloat16 or wider, within the bound.
A program may use at most 192 MiB of HBM per device.

```python
import math
import jax
import jax.numpy as jnp
from jax import lax

D = 4096
BLOCK_ORDER = 1024
LAYERS = 2
NBLK = 32
STRIP_ROWS = 256
SHARDS_PER_ROW = 1
OWNER_SLOTS = 5
SLOT_TOTAL = 40
BANDS = 8
SHARD_STRIPS = 4
N_DP = 4


def symmetric_draw(key, diagonal_lower, diagonal_upper, spread):
    jitter_key, diagonal_key = jax.random.split(key)
    jitter_portion = jax.random.normal(jitter_key, (SLOT_TOTAL, BLOCK_ORDER, BLOCK_ORDER), jnp.float32)
    diagonal_values = jnp.exp(jax.random.uniform(diagonal_key, (SLOT_TOTAL, BLOCK_ORDER), jnp.float32, math.log(diagonal_lower), math.log(diagonal_upper)))
    jitter_portion = jitter_portion * (spread / math.sqrt(BLOCK_ORDER))
    symmetric = (jitter_portion + jnp.swapaxes(jitter_portion, 1, 2)) * 0.70710678
    square_matrix = symmetric + jnp.eye(BLOCK_ORDER, dtype=jnp.float32)[None] * diagonal_values[:, :, None]
    return square_matrix.reshape(SLOT_TOTAL, SHARDS_PER_ROW, SHARD_STRIPS, STRIP_ROWS, BLOCK_ORDER)


def draw_slot_table(key, part):
    initial_key, later_key, third_key = jax.random.split(jax.random.fold_in(key, 11), 3)
    owner_ranks = jax.random.permutation(initial_key, SLOT_TOTAL).astype(jnp.int32)
    complete_owner = jax.random.randint(later_key, (), 0, SLOT_TOTAL // OWNER_SLOTS)
    slot_indices = jnp.arange(SLOT_TOTAL, dtype=jnp.int32)
    priority = jnp.where(slot_indices // OWNER_SLOTS == complete_owner, slot_indices % OWNER_SLOTS - OWNER_SLOTS, owner_ranks)
    ordering = jnp.argsort(priority, stable=True).astype(jnp.int32)
    chosen = ordering[:NBLK]
    shuffle = jax.random.permutation(third_key, NBLK)
    return chosen[shuffle].astype(jnp.int32)


def draw_left_gram_state(key, part):
    return symmetric_draw(jax.random.fold_in(key, 1), 0.5, 2.0, 0.3)


def draw_right_gram_state(key, part):
    return symmetric_draw(jax.random.fold_in(key, 2), 0.5, 2.0, 0.3)


def draw_left_inverse_root(key, part):
    return symmetric_draw(jax.random.fold_in(key, 3), 0.6, 1.5, 0.5).astype(jnp.bfloat16)


def draw_right_inverse_root(key, part):
    return symmetric_draw(jax.random.fold_in(key, 4), 0.6, 1.5, 0.5).astype(jnp.bfloat16)


def block_scale(own_key, dims, shards, smallest, high):
    factor_of, own = 1.0, jax.random.fold_in(own_key, 6)
    for position, blocks in shards:
        steps = jnp.exp(jax.random.uniform(jax.random.fold_in(own, position), (blocks,), jnp.float32, smallest / len(shards), high / len(shards)))
        factor_of = factor_of * jnp.repeat(steps, dims[position] // blocks).reshape([-1 if axis == position else 1 for axis in range(len(dims))])
    return factor_of


def gaussian(own_key, extent, width, most, shards=(), kind=jnp.bfloat16):
    loudness = block_scale(own_key, extent, shards, -0.22, 0.18) if shards else 1.0
    array = jax.random.normal(own_key, extent, jnp.float32) * width * loudness
    return jnp.minimum(jnp.maximum(array, -most), most).astype(kind)


def setup_inputs(seed: int = 0) -> dict:
    splits = jax.random.split(jax.random.key(seed), 7)
    replica_grads = gaussian(splits[0], (N_DP, LAYERS * D, D), 0.25, 4.0, ((0, 4), (1, 8)))
    slot_table = draw_slot_table(jax.random.fold_in(splits[6], 71), 0)
    left_gram_state = draw_left_gram_state(jax.random.fold_in(splits[6], 71), 0)
    right_gram_state = draw_right_gram_state(jax.random.fold_in(splits[6], 71), 0)
    left_inverse_root = draw_left_inverse_root(jax.random.fold_in(splits[6], 71), 0)
    right_inverse_root = draw_right_inverse_root(jax.random.fold_in(splits[6], 71), 0)
    return dict(replica_grads=replica_grads, slot_table=slot_table, left_gram_state=left_gram_state, right_gram_state=right_gram_state, left_inverse_root=left_inverse_root, right_inverse_root=right_inverse_root)


def reference(replica_grads, slot_table, left_gram_state, right_gram_state, left_inverse_root, right_inverse_root):
    per_band = D // BLOCK_ORDER
    summed = jnp.sum(replica_grads.astype(jnp.float32), axis=0).astype(jnp.bfloat16)
    blocks = summed.reshape(LAYERS * per_band, BLOCK_ORDER, per_band, BLOCK_ORDER).transpose(0, 2, 1, 3).reshape(NBLK, BLOCK_ORDER, BLOCK_ORDER)
    left_factors = left_gram_state.reshape(SLOT_TOTAL, BLOCK_ORDER, BLOCK_ORDER)
    right_factors = right_gram_state.reshape(SLOT_TOTAL, BLOCK_ORDER, BLOCK_ORDER)
    left_root_stack = left_inverse_root.reshape(SLOT_TOTAL, BLOCK_ORDER, BLOCK_ORDER)
    right_root_stack = right_inverse_root.reshape(SLOT_TOTAL, BLOCK_ORDER, BLOCK_ORDER)

    def one_block(index):
        slot = slot_table[index]
        gradient = blocks[index]
        left_next = left_factors[slot] + jnp.dot(gradient, gradient.T, preferred_element_type=jnp.float32) / BLOCK_ORDER
        right_next = right_factors[slot] + jnp.dot(gradient.T, gradient, preferred_element_type=jnp.float32) / BLOCK_ORDER
        mixed_rows = jnp.dot(left_root_stack[slot], gradient, preferred_element_type=jnp.float32).astype(jnp.bfloat16)
        outcome = jnp.dot(mixed_rows, right_root_stack[slot], preferred_element_type=jnp.float32).astype(jnp.bfloat16)
        return left_next, right_next, outcome

    left_next, right_next, outcomes = lax.map(one_block, jnp.arange(NBLK, dtype=jnp.int32))
    left_new = left_factors.at[slot_table].set(left_next).reshape(left_gram_state.shape)
    right_new = right_factors.at[slot_table].set(right_next).reshape(right_gram_state.shape)
    direction = outcomes.reshape(LAYERS * per_band, per_band, BLOCK_ORDER, BLOCK_ORDER).transpose(0, 2, 1, 3)
    direction = direction.reshape(BANDS, SHARD_STRIPS, STRIP_ROWS, D)
    return direction, left_new, right_new
```

```python
import functools

import jax
import jax.numpy as jnp
from jax import lax
from jax.experimental import pallas as pl
from jax.experimental.pallas import tpu as pltpu
from jax.sharding import PartitionSpec as P

MESH = pl.DeviceIdType.MESH
ANY = pl.BlockSpec(memory_space=pl.ANY)
VMEM = pl.BlockSpec(memory_space=pltpu.VMEM)
SMEM = pl.BlockSpec(memory_space=pltpu.SMEM)
F32 = jnp.float32
BF16 = jnp.bfloat16


def greet(peers):
    barrier = pltpu.get_barrier_semaphore()
    for peer in peers:
        pl.semaphore_signal(barrier, inc=1, device_id=peer, device_id_type=MESH)
    pl.semaphore_wait(barrier, len(peers))


def scatter_kernel(groups, shards, x_ref, o_ref, send_sem, recv_sem, own_sem):
    z, f = lax.axis_index("dp"), lax.axis_index("fsdp")
    peers = []
    for df in range(shards):
        for dz in range(groups):
            if df or dz:
                peers.append((lax.rem(z + dz, groups), lax.rem(f + df, shards)))
    me = z * shards + f
    own = pltpu.make_async_copy(x_ref.at[me], o_ref.at[me], own_sem)
    own.start()
    greet([{"dp": pz, "fsdp": pf} for pz, pf in peers])
    copies = []
    for k, (pz, pf) in enumerate(peers):
        copy = pltpu.make_async_remote_copy(
            src_ref=x_ref.at[pz * shards + pf],
            dst_ref=o_ref.at[me],
            send_sem=send_sem.at[k],
            recv_sem=recv_sem.at[k],
            device_id={"dp": pz, "fsdp": pf},
            device_id_type=MESH,
        )
        copy.start()
        copies.append(copy)
    own.wait()
    for copy in copies:
        copy.wait()


def scatter(x, groups, shards):
    count = groups * shards
    return pl.pallas_call(
        functools.partial(scatter_kernel, groups, shards),
        out_shape=jax.ShapeDtypeStruct(x.shape, x.dtype),
        in_specs=[ANY],
        out_specs=ANY,
        scratch_shapes=[
            pltpu.SemaphoreType.DMA((count - 1,)),
            pltpu.SemaphoreType.DMA((count - 1,)),
            pltpu.SemaphoreType.DMA,
        ],
        compiler_params=pltpu.CompilerParams(collective_id=0, has_side_effects=True),
    )(x)


def exchange_kernel(shards, x_ref, o_ref, send_sem, recv_sem, own_sem):
    f = lax.axis_index("fsdp")
    own = pltpu.make_async_copy(x_ref.at[f], o_ref.at[f], own_sem)
    own.start()
    peers = [lax.rem(f + d, shards) for d in range(1, shards)]
    greet([{"fsdp": p} for p in peers])
    copies = []
    for k, p in enumerate(peers):
        copy = pltpu.make_async_remote_copy(
            src_ref=x_ref.at[p],
            dst_ref=o_ref.at[f],
            send_sem=send_sem.at[k],
            recv_sem=recv_sem.at[k],
            device_id={"fsdp": p},
            device_id_type=MESH,
        )
        copy.start()
        copies.append(copy)
    own.wait()
    for copy in copies:
        copy.wait()


def exchange(x, shards, collective_id):
    return pl.pallas_call(
        functools.partial(exchange_kernel, shards),
        out_shape=jax.ShapeDtypeStruct(x.shape, x.dtype),
        in_specs=[ANY],
        out_specs=ANY,
        scratch_shapes=[
            pltpu.SemaphoreType.DMA((shards - 1,)),
            pltpu.SemaphoreType.DMA((shards - 1,)),
            pltpu.SemaphoreType.DMA,
        ],
        compiler_params=pltpu.CompilerParams(
            collective_id=collective_id, has_side_effects=True
        ),
    )(x)


def gather_kernel(
    groups, shards, sel_ref, root_ref, g_ref, r_ref, xs, xr, gs, gr, rs, rr, own_sem
):
    z, f = lax.axis_index("dp"), lax.axis_index("fsdp")
    up, down = lax.rem(z + 1, groups), lax.rem(z + groups - 1, groups)
    piece = sel_ref.shape[2]
    half = root_ref.shape[1] // 2
    own_root = pltpu.make_async_copy(root_ref, r_ref.at[z], own_sem.at[0])
    own_root.start()
    own_piece = pltpu.make_async_copy(
        sel_ref.at[f], g_ref.at[z, :, pl.ds(f * piece, piece), :], own_sem.at[1]
    )
    own_piece.start()
    peers = [lax.rem(f + d, shards) for d in range(1, shards)]
    greet([{"fsdp": p} for p in peers] + [{"dp": up}, {"dp": down}])

    def hop(buf, src, origin, part, way, send, recv, k):
        rows = pl.ds(part * half, half)
        return pltpu.make_async_remote_copy(
            src_ref=(buf.at[origin] if src is None else src).at[:, rows, :],
            dst_ref=buf.at[origin].at[:, rows, :],
            send_sem=send.at[k],
            recv_sem=recv.at[k],
            device_id={"dp": way},
            device_id_type=MESH,
        )

    def first(buf, src, send, recv):
        moves = [
            hop(buf, src, z, 0, up, send, recv, 0),
            hop(buf, src, z, 1, down, send, recv, 1),
            hop(buf, src, z, 1, up, send, recv, 2),
            hop(buf, src, z, 0, down, send, recv, 3),
        ]
        for move in moves:
            move.start()
        return moves

    def second(buf, send, recv):
        return [
            hop(buf, None, down, 0, up, send, recv, 4),
            hop(buf, None, up, 1, down, send, recv, 5),
        ]

    root_first = first(r_ref, root_ref, rs, rr)
    pieces = []
    for k, p in enumerate(peers):
        copy = pltpu.make_async_remote_copy(
            src_ref=sel_ref.at[p],
            dst_ref=g_ref.at[z, :, pl.ds(f * piece, piece), :],
            send_sem=xs.at[k],
            recv_sem=xr.at[k],
            device_id={"fsdp": p},
            device_id_type=MESH,
        )
        copy.start()
        pieces.append(copy)
    root_second = second(r_ref, rs, rr)
    for near, far in zip(root_first[:2], root_second):
        near.wait_recv()
        far.start()
    own_piece.wait()
    for copy in pieces:
        copy.wait()
    block_first = first(g_ref, None, gs, gr)
    block_second = second(g_ref, gs, gr)
    for near, far in zip(block_first[:2], block_second):
        near.wait_recv()
        far.start()
    for moves in (root_first, block_first):
        for k, move in enumerate(moves):
            if k >= 2:
                move.wait_recv()
            move.wait_send()
    for move in root_second + block_second:
        move.wait()
    own_root.wait()


def gather(sel, root, groups, shards):
    whole = jax.ShapeDtypeStruct((groups,) + root.shape, root.dtype)
    return pl.pallas_call(
        functools.partial(gather_kernel, groups, shards),
        out_shape=(whole, whole),
        in_specs=[ANY, ANY],
        out_specs=(ANY, ANY),
        scratch_shapes=[pltpu.SemaphoreType.DMA((shards - 1,))] * 2
        + [pltpu.SemaphoreType.DMA((6,))] * 4
        + [pltpu.SemaphoreType.DMA((2,))],
        compiler_params=pltpu.CompilerParams(collective_id=1, has_side_effects=True),
    )(sel, root)


def pick_blocks_kernel(groups, shards, slots, width, block_ref, occupied_ref, x_ref, o_ref):
    def body(s, carry):
        block = block_ref[s]
        band = block // (x_ref.shape[2] // width)
        column = pl.multiple_of(block % (x_ref.shape[2] // width) * width, width)
        total = x_ref[band, :, pl.ds(column, width)].astype(F32)
        for g in range(1, groups):
            total += x_ref[g * shards + band, :, pl.ds(column, width)].astype(F32)
        kept = jnp.where(occupied_ref[s] != 0, total, 0.0)
        o_ref[s] = kept.astype(o_ref.dtype)
        return carry

    lax.fori_loop(0, slots, body, 0)


def pick_blocks(block_of, occupied, x, groups, shards, slots, width):
    piece, model = x.shape[1:]
    step = 16 if piece % 16 == 0 else piece
    return pl.pallas_call(
        functools.partial(pick_blocks_kernel, groups, shards, slots, width),
        grid=(piece // step,),
        out_shape=jax.ShapeDtypeStruct((slots, piece, width), x.dtype),
        in_specs=[SMEM, SMEM, pl.BlockSpec((groups * shards, step, model), lambda i: (0, i, 0))],
        out_specs=pl.BlockSpec((slots, step, width), lambda i: (0, i, 0)),
    )(block_of, occupied, x)


def pick_home_kernel(per_band, slot_ref, x_ref, o_ref):
    width = x_ref.shape[2]

    def body(f, carry):
        for c in range(per_band):
            o_ref[f, :, c * width : (c + 1) * width] = x_ref[slot_ref[f * per_band + c]]
        return carry

    lax.fori_loop(0, o_ref.shape[0], body, 0)


def pick_home(slot_table, x, bands, per_band):
    slots, piece, width = x.shape
    return pl.pallas_call(
        functools.partial(pick_home_kernel, per_band),
        out_shape=jax.ShapeDtypeStruct((bands, piece, per_band * width), x.dtype),
        in_specs=[SMEM, VMEM],
        out_specs=VMEM,
    )(slot_table, x)


def step_kernel(place_ref, g_ref, r_ref, l_ref, ls_ref, rs_ref, d_ref, ln_ref, rn_ref):
    z = place_ref[0]
    size = g_ref.shape[3]
    rows = l_ref.shape[1]
    block = g_ref[:, 0].reshape(size, size)
    mine = g_ref[z, 0]
    columns = g_ref[:, 0, :, pl.ds(pl.multiple_of(z * rows, rows), rows)].reshape(size, rows)
    left = lax.dot_general(mine, block, (((1,), (1,)), ((), ())), preferred_element_type=F32)
    ln_ref[0] = ls_ref[0] + left / size
    right = lax.dot_general(columns, block, (((0,), (0,)), ((), ())), preferred_element_type=F32)
    rn_ref[0] = rs_ref[0] + right / size
    mixed = jnp.dot(l_ref[0], block, preferred_element_type=F32).astype(BF16)
    root = r_ref[:, 0].reshape(size, size)
    out = jnp.dot(mixed, root, preferred_element_type=F32).astype(d_ref.dtype)
    d_ref[:, 0] = out.reshape(d_ref.shape[0], d_ref.shape[2], size)


def step(place, g, r, left_root, left_state, right_state, shards):
    groups, slots, rows, size = g.shape
    piece = rows // shards
    whole = pl.BlockSpec((groups, 1, rows, size), lambda m: (0, m, 0, 0))
    strip = pl.BlockSpec((1, rows, size), lambda m: (m, 0, 0))
    state = jax.ShapeDtypeStruct((slots, rows, size), F32)
    return pl.pallas_call(
        step_kernel,
        grid=(slots,),
        out_shape=(jax.ShapeDtypeStruct((shards, slots, piece, size), BF16), state, state),
        in_specs=[SMEM, whole, whole, strip, strip, strip],
        out_specs=(pl.BlockSpec((shards, 1, piece, size), lambda m: (0, m, 0, 0)), strip, strip),
    )(place, g, r, left_root, left_state, right_state)


def by_pieces(replica_grads, slot_table, left_gram_state, right_gram_state, left_inverse_root, right_inverse_root):
    slots_here, _, _, rows, size = left_gram_state.shape
    band_rows, model_width = replica_grads.shape[1:]
    per_band = model_width // size
    shards, groups = lax.axis_size("fsdp"), lax.axis_size("dp")
    total_slots = shards * slots_here
    piece = rows // shards
    holder = slot_table[None, :] == jnp.arange(total_slots, dtype=jnp.int32)[:, None]
    occupied = jnp.any(holder, axis=1).astype(jnp.int32)
    numbers = jnp.arange(slot_table.shape[0], dtype=jnp.int32)
    block_of = jnp.sum(jnp.where(holder, numbers[None, :], 0), axis=1).astype(jnp.int32)

    arrived = scatter(
        replica_grads.reshape(groups * shards, piece, model_width), groups, shards
    )
    chosen = pick_blocks(block_of, occupied, arrived, groups, shards, total_slots, size)
    blocks, roots = gather(
        chosen.reshape(shards, slots_here, piece, size),
        right_inverse_root.reshape(slots_here, rows, size),
        groups,
        shards,
    )
    place = lax.axis_index("dp").astype(jnp.int32)[None]
    outcome, left_new, right_new = step(
        place,
        blocks,
        roots,
        left_inverse_root.reshape(slots_here, rows, size),
        left_gram_state.reshape(slots_here, rows, size),
        right_gram_state.reshape(slots_here, rows, size),
        shards,
    )
    returned = exchange(outcome, shards, 2)
    homeward = pick_home(
        slot_table, returned.reshape(total_slots, piece, size), shards, per_band
    )
    direction = exchange(homeward, shards, 3)
    return (
        direction.reshape(1, 1, rows, model_width),
        left_new.reshape(left_gram_state.shape),
        right_new.reshape(right_gram_state.shape),
    )


def fits_pieces(mesh_shape, grads, state):
    groups, shards = mesh_shape["dp"], mesh_shape["fsdp"]
    rows, size = state[3], state[4]
    return (
        groups == 4
        and state[1] == 1
        and grads[1] // shards == size
        and rows % (shards * 16) == 0
        and rows * groups == size
    )


def on_device(
    replica_grads,
    slot_table,
    left_gram_state,
    right_gram_state,
    left_inverse_root,
    right_inverse_root,
):
    slots_here = left_gram_state.shape[0]
    sub_blocks = left_gram_state.shape[1]
    strip_rows = left_gram_state.shape[3]
    block_size = left_gram_state.shape[4]
    band_rows = replica_grads.shape[1]
    model_width = replica_grads.shape[2]
    per_band = model_width // block_size
    shards = lax.axis_size("fsdp")
    groups = lax.axis_size("dp")
    total_slots = shards * slots_here
    block_count = slot_table.shape[0]
    band_index = lax.axis_index("fsdp")
    strip_index = lax.axis_index("dp")
    slot_indices = jnp.arange(total_slots, dtype=jnp.int32)
    summed = lax.psum_scatter(
        replica_grads[0].astype(jnp.float32).astype(jnp.bfloat16),
        "dp",
        scatter_dimension=0,
        tiled=True,
    )
    row_block = band_index * band_rows // block_size
    targets = lax.dynamic_slice_in_dim(slot_table, row_block * per_band, per_band, 0)
    chooser = (targets[:, None] == slot_indices[None, :]).astype(jnp.bfloat16)
    own_slots = band_index * slots_here + jnp.arange(slots_here, dtype=jnp.int32)
    holder = slot_table[None, :] == own_slots[:, None]
    occupied = jnp.any(holder, axis=1)
    block_of = jnp.sum(
        jnp.where(holder, jnp.arange(block_count, dtype=jnp.int32)[None, :], 0), axis=1
    )
    first_band = block_of // per_band * sub_blocks
    col_block = block_of % per_band
    all_bands = lax.all_gather(summed[None], "fsdp", axis=0, tiled=True)
    owned_rows = jax.vmap(
        lambda offset, column: lax.dynamic_slice(
            all_bands, (offset, 0, column * block_size), (sub_blocks, strip_rows, block_size)
        )
    )(first_band, col_block)
    owned_rows = owned_rows * occupied[:, None, None, None].astype(jnp.bfloat16)
    owned_rows = owned_rows.reshape(slots_here, sub_blocks, 1, strip_rows, block_size)
    entire = lax.all_gather(owned_rows, "dp", axis=2, tiled=True).reshape(
        slots_here, block_size, block_size
    )
    my_rows = owned_rows.reshape(slots_here, sub_blocks * strip_rows, block_size)
    left_gram = jnp.einsum("mrc,mnc->mrn", my_rows, entire, preferred_element_type=jnp.float32)
    left_new = left_gram_state + (left_gram / block_size).reshape(left_gram_state.shape)
    my_columns = lax.dynamic_index_in_dim(
        entire.reshape(slots_here, block_size, sub_blocks, groups, strip_rows),
        strip_index,
        3,
        keepdims=False,
    )
    my_columns = my_columns.reshape(slots_here, block_size, sub_blocks * strip_rows)
    right_gram = jnp.einsum("mnr,mnc->mrc", my_columns, entire, preferred_element_type=jnp.float32)
    right_new = right_gram_state + (right_gram / block_size).reshape(right_gram_state.shape)
    left_rows = left_inverse_root.reshape(slots_here, sub_blocks * strip_rows, block_size)
    mixed_rows = jnp.einsum(
        "mrn,mnc->mrc", left_rows, entire, preferred_element_type=jnp.float32
    ).astype(jnp.bfloat16)
    mixed_split = mixed_rows.reshape(
        slots_here, sub_blocks * strip_rows, sub_blocks, groups, strip_rows
    )
    result = jnp.einsum(
        "mrqjt,mqjtc->mrc",
        mixed_split,
        lax.all_gather(right_inverse_root, "dp", axis=2, tiled=True),
        preferred_element_type=jnp.float32,
    )
    outcome = result.astype(jnp.bfloat16).reshape(slots_here, sub_blocks, strip_rows, block_size)
    homeward = jax.vmap(
        lambda portion, offset: lax.dynamic_update_slice_in_dim(
            jnp.zeros((shards, strip_rows, block_size), jnp.bfloat16), portion, offset, 0
        ),
        out_axes=1,
    )(outcome, first_band)
    returned = lax.all_to_all(homeward, "fsdp", split_axis=0, concat_axis=0, tiled=True)
    picked = jnp.einsum(
        "cn,ntb->tcb",
        chooser,
        returned.reshape(total_slots, strip_rows, block_size),
        preferred_element_type=jnp.float32,
    ).astype(jnp.bfloat16)
    direction = picked.reshape(1, 1, strip_rows, model_width)
    return (direction, left_new, right_new)


def solution(mesh):
    placed = (
        P("dp", "fsdp", None),
        P(),
        P("fsdp", None, "dp", None, None),
        P("fsdp", None, "dp", None, None),
        P("fsdp", None, "dp", None, None),
        P("fsdp", None, "dp", None, None),
    )
    places = (
        P("fsdp", "dp", None, None),
        P("fsdp", None, "dp", None, None),
        P("fsdp", None, "dp", None, None),
    )

    def run(*args):
        grads, _, state = args[:3]
        fits = fits_pieces(mesh.shape, grads.shape, state.shape)
        mapped = jax.shard_map(
            by_pieces if fits else on_device,
            mesh=mesh,
            in_specs=placed,
            out_specs=places,
            check_vma=False,
        )
        return mapped(*args)

    return run
```

```python
import functools

import jax
import jax.numpy as jnp
from jax import lax
from jax.experimental import pallas as pl
from jax.experimental.pallas import tpu as pltpu
from jax.sharding import PartitionSpec as P

MESH = pl.DeviceIdType.MESH
ANY = pl.BlockSpec(memory_space=pl.ANY)
VMEM = pl.BlockSpec(memory_space=pltpu.VMEM)
SMEM = pl.BlockSpec(memory_space=pltpu.SMEM)
F32 = jnp.float32
BF16 = jnp.bfloat16


def greet(peers):
    barrier = pltpu.get_barrier_semaphore()
    for peer in peers:
        pl.semaphore_signal(barrier, inc=1, device_id=peer, device_id_type=MESH)
    pl.semaphore_wait(barrier, len(peers))


def chain_start(groups, z, buf, src, send, recv):
    def move(origin, way, side, d):
        origin = jnp.clip(origin, 0, groups - 1)
        return pltpu.make_async_remote_copy(
            src_ref=src if d == 0 and src is not None else buf.at[origin],
            dst_ref=buf.at[origin],
            send_sem=send.at[side, d],
            recv_sem=recv.at[side, d],
            device_id={"dp": jnp.clip(way, 0, groups - 1)},
            device_id_type=MESH,
        )

    sides = ((0, -1), (1, 1))

    def send_on(d):
        for side, sign in sides:
            origin, way = z + sign * d, z - sign
            inside = (origin >= 0) & (origin < groups) & (way >= 0) & (way < groups)

            @pl.when(inside)
            def _():
                move(origin, way, side, d).start()

    def relay():
        for d in range(1, groups):
            for side, sign in sides:
                origin = z + sign * d

                @pl.when((origin >= 0) & (origin < groups))
                def _():
                    move(origin, z, side, d - 1).wait_recv()

            if d < groups - 1:
                send_on(d)

    def finish():
        for d in range(groups - 1):
            for side, sign in sides:
                origin, way = z + sign * d, z - sign
                inside = (origin >= 0) & (origin < groups) & (way >= 0) & (way < groups)

                @pl.when(inside)
                def _():
                    move(origin, way, side, d).wait_send()

    send_on(0)
    return relay, finish


def scatter_kernel(
    groups, shards, x_ref, root_ref, o_ref, near_ref, send_sem, recv_sem, rs, rr, own_sem
):
    z, f = lax.axis_index("dp"), lax.axis_index("fsdp")
    peers = []
    for df in range(shards):
        for dz in range(groups):
            if df or dz:
                peers.append((lax.rem(z + dz, groups), lax.rem(f + df, shards)))
    me = z * shards + f
    own = pltpu.make_async_copy(x_ref.at[me], o_ref.at[me], own_sem)
    own.start()
    greet([{"dp": pz, "fsdp": pf} for pz, pf in peers])
    copies = []
    for k, (pz, pf) in enumerate(peers):
        copy = pltpu.make_async_remote_copy(
            src_ref=x_ref.at[pz * shards + pf],
            dst_ref=o_ref.at[me],
            send_sem=send_sem.at[k],
            recv_sem=recv_sem.at[k],
            device_id={"dp": pz, "fsdp": pf},
            device_id_type=MESH,
        )
        copy.start()
        copies.append(copy)
    root = pltpu.make_async_remote_copy(
        src_ref=root_ref,
        dst_ref=near_ref,
        send_sem=rs,
        recv_sem=rr,
        device_id={"dp": z + 1 - 2 * lax.rem(z, 2)},
        device_id_type=MESH,
    )
    root.start()
    own.wait()
    for copy in copies:
        copy.wait()
    root.wait()


def scatter(x, root, groups, shards):
    count = groups * shards
    return pl.pallas_call(
        functools.partial(scatter_kernel, groups, shards),
        out_shape=(jax.ShapeDtypeStruct(x.shape, x.dtype), jax.ShapeDtypeStruct(root.shape, root.dtype)),
        in_specs=[ANY, ANY],
        out_specs=(ANY, ANY),
        scratch_shapes=[pltpu.SemaphoreType.DMA((count - 1,))] * 2
        + [pltpu.SemaphoreType.DMA] * 3,
        compiler_params=pltpu.CompilerParams(collective_id=0, has_side_effects=True),
    )(x, root)


def exchange_kernel(shards, x_ref, o_ref, send_sem, recv_sem, own_sem):
    f = lax.axis_index("fsdp")
    own = pltpu.make_async_copy(x_ref.at[f], o_ref.at[f], own_sem)
    own.start()
    peers = [lax.rem(f + d, shards) for d in range(1, shards)]
    greet([{"fsdp": p} for p in peers])
    copies = []
    for k, p in enumerate(peers):
        copy = pltpu.make_async_remote_copy(
            src_ref=x_ref.at[p],
            dst_ref=o_ref.at[f],
            send_sem=send_sem.at[k],
            recv_sem=recv_sem.at[k],
            device_id={"fsdp": p},
            device_id_type=MESH,
        )
        copy.start()
        copies.append(copy)
    own.wait()
    for copy in copies:
        copy.wait()


def exchange(x, shards, collective_id):
    return pl.pallas_call(
        functools.partial(exchange_kernel, shards),
        out_shape=jax.ShapeDtypeStruct(x.shape, x.dtype),
        in_specs=[ANY],
        out_specs=ANY,
        scratch_shapes=[
            pltpu.SemaphoreType.DMA((shards - 1,)),
            pltpu.SemaphoreType.DMA((shards - 1,)),
            pltpu.SemaphoreType.DMA,
        ],
        compiler_params=pltpu.CompilerParams(
            collective_id=collective_id, has_side_effects=True
        ),
    )(x)


def gather_kernel(
    groups, shards, sel_ref, root_ref, near_ref, g_ref, r_ref, xs, xr, gs, gr, rs, rr, own_sem
):
    z, f = lax.axis_index("dp"), lax.axis_index("fsdp")
    piece = sel_ref.shape[2]
    pair = z + 1 - 2 * lax.rem(z, 2)
    middle = (z > 0) & (z < groups - 1)
    across = groups - 1 - z
    far = jnp.where(middle, across, groups - 1 - pair)
    far_pair = far + 1 - 2 * lax.rem(far, 2)
    own = pltpu.make_async_copy(
        sel_ref.at[f], g_ref.at[z, :, pl.ds(f * piece, piece), :], own_sem.at[0]
    )
    own.start()
    own_root = pltpu.make_async_copy(root_ref, r_ref.at[z], own_sem.at[1])
    own_root.start()
    near_root = pltpu.make_async_copy(near_ref, r_ref.at[pair], own_sem.at[2])
    near_root.start()

    def hand(src, row, way, k, sent):
        return pltpu.make_async_remote_copy(
            src_ref=src,
            dst_ref=r_ref.at[row],
            send_sem=rs.at[sent],
            recv_sem=rr.at[k],
            device_id={"dp": way},
            device_id_type=MESH,
        )

    swaps = [hand(root_ref, z, across, 0, 0), hand(near_ref, pair, across, 1, 1)]
    passes = [
        hand(r_ref.at[far], far, pair, 0, 2),
        hand(r_ref.at[far_pair], far_pair, pair, 1, 3),
    ]
    peers = [lax.rem(f + d, shards) for d in range(1, shards)]
    near = [lax.rem(z + 1, groups), lax.rem(z + groups - 1, groups)]
    greet([{"fsdp": p} for p in peers] + [{"dp": p} for p in near])

    @pl.when(middle)
    def _():
        for swap in swaps:
            swap.start()

    copies = []
    for k, p in enumerate(peers):
        copy = pltpu.make_async_remote_copy(
            src_ref=sel_ref.at[p],
            dst_ref=g_ref.at[z, :, pl.ds(f * piece, piece), :],
            send_sem=xs.at[k],
            recv_sem=xr.at[k],
            device_id={"fsdp": p},
            device_id_type=MESH,
        )
        copy.start()
        copies.append(copy)
    for onward in passes:
        onward.wait_recv()

        @pl.when(middle)
        def _():
            onward.start()

    own.wait()
    for copy in copies:
        copy.wait()
    relay, finish = chain_start(groups, z, g_ref, None, gs, gr)
    relay()
    finish()

    @pl.when(middle)
    def _():
        for move in swaps + passes:
            move.wait_send()

    own_root.wait()
    near_root.wait()


def gather(sel, root, near, groups, shards):
    slots, piece, size = sel.shape[1:]
    whole = jax.ShapeDtypeStruct((groups, slots, shards * piece, size), sel.dtype)
    return pl.pallas_call(
        functools.partial(gather_kernel, groups, shards),
        out_shape=(whole, whole),
        in_specs=[ANY] * 3,
        out_specs=(ANY, ANY),
        scratch_shapes=[pltpu.SemaphoreType.DMA((shards - 1,))] * 2
        + [pltpu.SemaphoreType.DMA((2, groups - 1))] * 2
        + [pltpu.SemaphoreType.DMA((4,)), pltpu.SemaphoreType.DMA((2,))]
        + [pltpu.SemaphoreType.DMA((3,))],
        compiler_params=pltpu.CompilerParams(collective_id=1, has_side_effects=True),
    )(sel, root, near)


def pick_blocks_kernel(groups, shards, slots, width, block_ref, occupied_ref, x_ref, o_ref):
    def body(s, carry):
        block = block_ref[s]
        band = block // (x_ref.shape[2] // width)
        column = pl.multiple_of(block % (x_ref.shape[2] // width) * width, width)
        total = x_ref[band, :, pl.ds(column, width)].astype(F32)
        for g in range(1, groups):
            total += x_ref[g * shards + band, :, pl.ds(column, width)].astype(F32)
        kept = jnp.where(occupied_ref[s] != 0, total, 0.0)
        o_ref[s] = kept.astype(o_ref.dtype)
        return carry

    lax.fori_loop(0, slots, body, 0)


def pick_blocks(block_of, occupied, x, groups, shards, slots, width):
    piece, model = x.shape[1:]
    step = 16 if piece % 16 == 0 else piece
    return pl.pallas_call(
        functools.partial(pick_blocks_kernel, groups, shards, slots, width),
        grid=(piece // step,),
        out_shape=jax.ShapeDtypeStruct((slots, piece, width), x.dtype),
        in_specs=[SMEM, SMEM, pl.BlockSpec((groups * shards, step, model), lambda i: (0, i, 0))],
        out_specs=pl.BlockSpec((slots, step, width), lambda i: (0, i, 0)),
    )(block_of, occupied, x)


def pick_home_kernel(per_band, slot_ref, x_ref, o_ref):
    width = x_ref.shape[2]

    def body(f, carry):
        for c in range(per_band):
            o_ref[f, :, c * width : (c + 1) * width] = x_ref[slot_ref[f * per_band + c]]
        return carry

    lax.fori_loop(0, o_ref.shape[0], body, 0)


def pick_home(slot_table, x, bands, per_band):
    slots, piece, width = x.shape
    return pl.pallas_call(
        functools.partial(pick_home_kernel, per_band),
        out_shape=jax.ShapeDtypeStruct((bands, piece, per_band * width), x.dtype),
        in_specs=[SMEM, VMEM],
        out_specs=VMEM,
    )(slot_table, x)


def step_kernel(place_ref, g_ref, r_ref, l_ref, ls_ref, rs_ref, d_ref, ln_ref, rn_ref):
    z = place_ref[0]
    size = g_ref.shape[3]
    rows = l_ref.shape[1]
    block = g_ref[:, 0].reshape(size, size)
    mine = g_ref[z, 0]
    columns = g_ref[:, 0, :, pl.ds(pl.multiple_of(z * rows, rows), rows)].reshape(size, rows)
    left = lax.dot_general(mine, block, (((1,), (1,)), ((), ())), preferred_element_type=F32)
    ln_ref[0] = ls_ref[0] + left / size
    right = lax.dot_general(columns, block, (((0,), (0,)), ((), ())), preferred_element_type=F32)
    rn_ref[0] = rs_ref[0] + right / size
    mixed = jnp.dot(l_ref[0], block, preferred_element_type=F32).astype(BF16)
    root = r_ref[:, 0].reshape(size, size)
    out = jnp.dot(mixed, root, preferred_element_type=F32).astype(d_ref.dtype)
    d_ref[:, 0] = out.reshape(d_ref.shape[0], d_ref.shape[2], size)


def step(place, g, r, left_root, left_state, right_state, shards):
    groups, slots, rows, size = g.shape
    piece = rows // shards
    whole = pl.BlockSpec((groups, 1, rows, size), lambda m: (0, m, 0, 0))
    strip = pl.BlockSpec((1, rows, size), lambda m: (m, 0, 0))
    state = jax.ShapeDtypeStruct((slots, rows, size), F32)
    return pl.pallas_call(
        step_kernel,
        grid=(slots,),
        out_shape=(jax.ShapeDtypeStruct((shards, slots, piece, size), BF16), state, state),
        in_specs=[SMEM, whole, whole, strip, strip, strip],
        out_specs=(pl.BlockSpec((shards, 1, piece, size), lambda m: (0, m, 0, 0)), strip, strip),
    )(place, g, r, left_root, left_state, right_state)


def by_pieces(replica_grads, slot_table, left_gram_state, right_gram_state, left_inverse_root, right_inverse_root):
    slots_here, _, _, rows, size = left_gram_state.shape
    band_rows, model_width = replica_grads.shape[1:]
    per_band = model_width // size
    shards, groups = lax.axis_size("fsdp"), lax.axis_size("dp")
    total_slots = shards * slots_here
    piece = rows // shards
    holder = slot_table[None, :] == jnp.arange(total_slots, dtype=jnp.int32)[:, None]
    occupied = jnp.any(holder, axis=1).astype(jnp.int32)
    numbers = jnp.arange(slot_table.shape[0], dtype=jnp.int32)
    block_of = jnp.sum(jnp.where(holder, numbers[None, :], 0), axis=1).astype(jnp.int32)

    own_roots = right_inverse_root.reshape(slots_here, rows, size)
    arrived, near_roots = scatter(
        replica_grads.reshape(groups * shards, piece, model_width),
        own_roots,
        groups,
        shards,
    )
    chosen = pick_blocks(block_of, occupied, arrived, groups, shards, total_slots, size)
    blocks, roots = gather(
        chosen.reshape(shards, slots_here, piece, size), own_roots, near_roots, groups, shards
    )
    place = lax.axis_index("dp").astype(jnp.int32)[None]
    outcome, left_new, right_new = step(
        place,
        blocks,
        roots,
        left_inverse_root.reshape(slots_here, rows, size),
        left_gram_state.reshape(slots_here, rows, size),
        right_gram_state.reshape(slots_here, rows, size),
        shards,
    )
    returned = exchange(outcome, shards, 2)
    homeward = pick_home(
        slot_table, returned.reshape(total_slots, piece, size), shards, per_band
    )
    direction = exchange(homeward, shards, 3)
    return (
        direction.reshape(1, 1, rows, model_width),
        left_new.reshape(left_gram_state.shape),
        right_new.reshape(right_gram_state.shape),
    )


def fits_pieces(mesh_shape, grads, state):
    groups, shards = mesh_shape["dp"], mesh_shape["fsdp"]
    rows, size = state[3], state[4]
    return (
        groups == 4
        and state[1] == 1
        and grads[1] // shards == size
        and rows % (shards * 16) == 0
        and rows * groups == size
    )


def on_device(
    replica_grads,
    slot_table,
    left_gram_state,
    right_gram_state,
    left_inverse_root,
    right_inverse_root,
):
    slots_here = left_gram_state.shape[0]
    sub_blocks = left_gram_state.shape[1]
    strip_rows = left_gram_state.shape[3]
    block_size = left_gram_state.shape[4]
    band_rows = replica_grads.shape[1]
    model_width = replica_grads.shape[2]
    per_band = model_width // block_size
    shards = lax.axis_size("fsdp")
    groups = lax.axis_size("dp")
    total_slots = shards * slots_here
    block_count = slot_table.shape[0]
    band_index = lax.axis_index("fsdp")
    strip_index = lax.axis_index("dp")
    slot_indices = jnp.arange(total_slots, dtype=jnp.int32)
    summed = lax.psum_scatter(
        replica_grads[0].astype(jnp.float32).astype(jnp.bfloat16),
        "dp",
        scatter_dimension=0,
        tiled=True,
    )
    row_block = band_index * band_rows // block_size
    targets = lax.dynamic_slice_in_dim(slot_table, row_block * per_band, per_band, 0)
    chooser = (targets[:, None] == slot_indices[None, :]).astype(jnp.bfloat16)
    own_slots = band_index * slots_here + jnp.arange(slots_here, dtype=jnp.int32)
    holder = slot_table[None, :] == own_slots[:, None]
    occupied = jnp.any(holder, axis=1)
    block_of = jnp.sum(
        jnp.where(holder, jnp.arange(block_count, dtype=jnp.int32)[None, :], 0), axis=1
    )
    first_band = block_of // per_band * sub_blocks
    col_block = block_of % per_band
    all_bands = lax.all_gather(summed[None], "fsdp", axis=0, tiled=True)
    owned_rows = jax.vmap(
        lambda offset, column: lax.dynamic_slice(
            all_bands, (offset, 0, column * block_size), (sub_blocks, strip_rows, block_size)
        )
    )(first_band, col_block)
    owned_rows = owned_rows * occupied[:, None, None, None].astype(jnp.bfloat16)
    owned_rows = owned_rows.reshape(slots_here, sub_blocks, 1, strip_rows, block_size)
    entire = lax.all_gather(owned_rows, "dp", axis=2, tiled=True).reshape(
        slots_here, block_size, block_size
    )
    my_rows = owned_rows.reshape(slots_here, sub_blocks * strip_rows, block_size)
    left_gram = jnp.einsum("mrc,mnc->mrn", my_rows, entire, preferred_element_type=jnp.float32)
    left_new = left_gram_state + (left_gram / block_size).reshape(left_gram_state.shape)
    my_columns = lax.dynamic_index_in_dim(
        entire.reshape(slots_here, block_size, sub_blocks, groups, strip_rows),
        strip_index,
        3,
        keepdims=False,
    )
    my_columns = my_columns.reshape(slots_here, block_size, sub_blocks * strip_rows)
    right_gram = jnp.einsum("mnr,mnc->mrc", my_columns, entire, preferred_element_type=jnp.float32)
    right_new = right_gram_state + (right_gram / block_size).reshape(right_gram_state.shape)
    left_rows = left_inverse_root.reshape(slots_here, sub_blocks * strip_rows, block_size)
    mixed_rows = jnp.einsum(
        "mrn,mnc->mrc", left_rows, entire, preferred_element_type=jnp.float32
    ).astype(jnp.bfloat16)
    mixed_split = mixed_rows.reshape(
        slots_here, sub_blocks * strip_rows, sub_blocks, groups, strip_rows
    )
    result = jnp.einsum(
        "mrqjt,mqjtc->mrc",
        mixed_split,
        lax.all_gather(right_inverse_root, "dp", axis=2, tiled=True),
        preferred_element_type=jnp.float32,
    )
    outcome = result.astype(jnp.bfloat16).reshape(slots_here, sub_blocks, strip_rows, block_size)
    homeward = jax.vmap(
        lambda portion, offset: lax.dynamic_update_slice_in_dim(
            jnp.zeros((shards, strip_rows, block_size), jnp.bfloat16), portion, offset, 0
        ),
        out_axes=1,
    )(outcome, first_band)
    returned = lax.all_to_all(homeward, "fsdp", split_axis=0, concat_axis=0, tiled=True)
    picked = jnp.einsum(
        "cn,ntb->tcb",
        chooser,
        returned.reshape(total_slots, strip_rows, block_size),
        preferred_element_type=jnp.float32,
    ).astype(jnp.bfloat16)
    direction = picked.reshape(1, 1, strip_rows, model_width)
    return (direction, left_new, right_new)


def solution(mesh):
    placed = (
        P("dp", "fsdp", None),
        P(),
        P("fsdp", None, "dp", None, None),
        P("fsdp", None, "dp", None, None),
        P("fsdp", None, "dp", None, None),
        P("fsdp", None, "dp", None, None),
    )
    places = (
        P("fsdp", "dp", None, None),
        P("fsdp", None, "dp", None, None),
        P("fsdp", None, "dp", None, None),
    )

    def run(*args):
        grads, _, state = args[:3]
        fits = fits_pieces(mesh.shape, grads.shape, state.shape)
        mapped = jax.shard_map(
            by_pieces if fits else on_device,
            mesh=mesh,
            in_specs=placed,
            out_specs=places,
            check_vma=False,
        )
        return mapped(*args)

    return run
```
